256 devices in a mesh: gx: 8 (over y, core), gy: 4 (over z_lo), gz: 8 (over x, z_hi).
Axes of the slice: x: 4, y: 4, z: 8 (z_hi: 2, z_lo: 4; z = z_hi * 4 + z_lo), core: 2. Of those that a mesh axis runs over, the one named last changes fastest.
Arguments:
- stream: bfloat16 [65536, 8192], P(('gx', 'gy', 'gz')), may hold values from -4 to 4
- segment_ids: int32 [65536], P(('gx', 'gy', 'gz')), may hold values from 0 to 65535, as said below
- positions: int32 [65536], P(('gx', 'gy', 'gz')), may hold values from 0 to 255, as said below
- norm_gain: bfloat16 [1, 8192], P(None, ('gx', 'gy', 'gz')), may hold values from 0.099609375 to 1.8984375
- q_weight: bfloat16 [1, 8192, 512], P(None, ('gx', 'gy', 'gz')), as said below
- k_weight: bfloat16 [1, 8192, 128], P(None, ('gx', 'gy', 'gz')), as said below
- v_weight: bfloat16 [1, 8192, 128], P(None, ('gx', 'gy', 'gz')), may hold values from -0.0625 to 0.0625
- o_weight: bfloat16 [1, 512, 8192], P(None, None, ('gx', 'gy', 'gz')), may hold values from -0.25 to 0.25
Outputs:
- result: bfloat16 [65536, 8192], P(('gx', 'gy', 'gz'))
The draws below stay inside these ranges and needn't reach their ends.
Inputs may be any that keep to these rules, and one draw needn't show every extreme that they name: `segment_ids`: each token's id is the index of its document's first token, so ids never fall along the tokens; every document lies inside one aligned block of 256 tokens, every block starts a new document, and the last token is a document of its own. `positions`: counts from 0 at a document's first token and rises by one per token. `q_weight`: A projection scaled by its fan-in. `k_weight`: A projection scaled by its fan-in.
All inputs are finite; a program needn't handle non-finite values.
Results may differ from the reference program's by a relative error of at most 0.0064.
Values may be sent and summed in bfloat16 or wider, within the bound.
No kernel may reach another device: no remote copies, remote signals or barrier semaphores. Data moves between devices by JAX's collectives and lax.ppermute only.
A program may use at most 128 MiB of HBM per device.

```python
import math
import jax
import jax.numpy as jnp
from jax import lax

D = 8192
HD = 128
QH = 4
LAYERS = 1
TOK_DEV = 256
TOKENS = 65536


def segment_plan(key):
    base = jax.random.fold_in(key, 301)
    marks = jax.random.randint(base, (TOKENS,), 0, 80)
    index = jnp.arange(TOKENS, dtype=jnp.int32)
    starts = (marks == 0) | (index % TOK_DEV == 0) | (index == TOKENS - 1)
    begin = lax.cummax(jnp.where(starts, index, 0), axis=0)
    return (begin.astype(jnp.int32), (index - begin).astype(jnp.int32))


def draw_segment_ids(key, part):
    return segment_plan(key)[0]


def draw_positions(key, part):
    return segment_plan(key)[1]


def row_scales(key):
    return jnp.exp(jax.random.uniform(jax.random.fold_in(key, 411), (LAYERS, D, 1), jnp.float32, -0.7, 0.7))


def key_plan(key):
    noise_key = jax.random.fold_in(key, 401)
    base = jax.random.normal(noise_key, (LAYERS, D, HD), jnp.float32) * D ** (-0.5) * row_scales(key)
    return base


def draw_k_weight(key, part):
    return key_plan(key).astype(jnp.bfloat16)


def draw_q_weight(key, part):
    noise = jax.random.normal(jax.random.fold_in(key, 421), (LAYERS, D, QH * HD), jnp.float32) * D ** (-0.5) * row_scales(key)
    return noise.astype(jnp.bfloat16)


def levels(own_key, shape, shards, smallest, high):
    factor_of = 1.0
    for position, parts in shards:
        draws = jax.random.uniform(jax.random.fold_in(jax.random.fold_in(own_key, 6), position), (parts,), jnp.float32, smallest / len(shards), high / len(shards))
        factor_of = factor_of * jnp.repeat(jnp.exp(draws), shape[position] // parts).reshape((-1,) + (1,) * (len(shape) - 1 - position))
    return factor_of


def gaussian(rng, shape, scale, bound, pieces=(), held_as=jnp.bfloat16):
    factor_of = levels(rng, shape, pieces, -0.22, 0.18) if pieces else 1.0
    values = jax.random.normal(rng, shape, jnp.float32) * scale * factor_of
    return jnp.minimum(jnp.maximum(values, -bound), bound).astype(held_as)


def setup_inputs(seed: int = 0) -> dict:
    key_list = jax.random.split(jax.random.key(seed), 9)
    stream = gaussian(key_list[0], (TOKENS, D), 0.5, 4.0, ((0, 256),))
    segment_ids = draw_segment_ids(jax.random.fold_in(key_list[8], 71), 0)
    positions = draw_positions(jax.random.fold_in(key_list[8], 71), 0)
    norm_gain = jnp.clip(1.0 + 0.18 * jax.random.normal(key_list[3], (LAYERS, D), jnp.float32), 0.099609375, 1.8984375).astype(jnp.bfloat16)
    q_weight = draw_q_weight(jax.random.fold_in(key_list[8], 71), 0)
    k_weight = draw_k_weight(jax.random.fold_in(key_list[8], 71), 0)
    v_weight = gaussian(key_list[6], (LAYERS, D, HD), D ** -0.5, 0.0625, ((1, 256),))
    o_weight = gaussian(key_list[7], (LAYERS, QH * HD, D), (QH * HD) ** -0.5, 0.25, ((2, 256),))
    return {"stream": stream, "segment_ids": segment_ids, "positions": positions, "norm_gain": norm_gain, "q_weight": q_weight, "k_weight": k_weight, "v_weight": v_weight, "o_weight": o_weight}


def rotate(values, positions):
    width = values.shape[-1]
    half = width // 2
    freqs = jnp.exp(-math.log(500000.0) * jnp.arange(half, dtype=jnp.float32) * 2.0 / width)
    angles = positions.astype(jnp.float32)[:, None] * freqs[None, :]
    cosine = jnp.concatenate([jnp.cos(angles), jnp.cos(angles)], -1)[:, None, :]
    sine = jnp.concatenate([jnp.sin(angles), jnp.sin(angles)], -1)[:, None, :]
    turned = jnp.concatenate([-values[..., half:], values[..., :half]], -1)
    return values * cosine + turned * sine

def attend(queries, keys, values, segment_ids, positions):
    count = queries.shape[0]
    scores = jnp.einsum('thd,sd->hts', queries.astype(jnp.float32), keys.astype(jnp.float32)) / math.sqrt(keys.shape[-1])
    allowed = (segment_ids[:, None] == segment_ids[None, :]) & (positions[None, :] <= positions[:, None])
    scores = jnp.where(allowed[None], scores, -1e+30)
    peak = lax.optimization_barrier(jnp.max(scores, -1, keepdims=True))
    expd = jnp.exp(scores - peak)
    probs = (expd / lax.optimization_barrier(jnp.sum(expd, -1, keepdims=True))).astype(jnp.bfloat16)
    mixed = jnp.einsum('hts,sd->thd', probs.astype(jnp.float32), values.astype(jnp.float32))
    return mixed.astype(jnp.bfloat16).reshape(count, -1)

def run_block(block, segment_ids, positions, norm_gain, q_weight, k_weight, v_weight, o_weight):
    count = block.shape[0]
    current = block
    for layer in range(LAYERS):
        widened = lax.optimization_barrier(current).astype(jnp.float32)
        inverse = lax.rsqrt(lax.optimization_barrier(jnp.mean(widened * widened, -1, keepdims=True)) + 1e-05)
        normed = (widened * inverse * norm_gain[layer].astype(jnp.float32)).astype(jnp.bfloat16)
        query_raw = jnp.dot(normed, q_weight[layer], preferred_element_type=jnp.float32)
        key_raw = jnp.dot(normed, k_weight[layer], preferred_element_type=jnp.float32)
        value_raw = jnp.dot(normed, v_weight[layer], preferred_element_type=jnp.float32)
        queries = rotate(query_raw.reshape(count, QH, HD), positions).astype(jnp.bfloat16)
        keys = rotate(key_raw[:, None, :], positions)[:, 0, :].astype(jnp.bfloat16)
        values = value_raw.astype(jnp.bfloat16)
        mixed = attend(queries, keys, values, segment_ids, positions)
        branch = jnp.dot(mixed, o_weight[layer], preferred_element_type=jnp.float32)
        current = (widened + branch).astype(jnp.bfloat16)
    return current

def reference(stream, segment_ids, positions, norm_gain, q_weight, k_weight, v_weight, o_weight):
    blocks = TOKENS // TOK_DEV

    def one(item):
        return run_block(item[0], item[1], item[2], norm_gain, q_weight, k_weight, v_weight, o_weight)
    result = lax.map(one, (stream.reshape(blocks, TOK_DEV, D), segment_ids.reshape(blocks, TOK_DEV), positions.reshape(blocks, TOK_DEV)), batch_size=8)
    return result.reshape(TOKENS, D)
```

```python
import functools
import math

import jax
import jax.numpy as jnp
from jax import lax
from jax.experimental import pallas as pl
from jax.experimental.pallas import tpu as pltpu
from jax.sharding import Mesh, PartitionSpec as P

AXES = ("y", "c", "zl", "x", "zh")
NY, NC, NZL, NX, NZH = 4, 2, 4, 4, 2
HD = 128
ROWS = 32
T = 256


def rope(h, cos, sin):
    return h * cos + pltpu.roll(h, HD // 2, 1) * sin


def attend_kernel(x_ref, w0_ref, w1_ref, w2_ref, inv_ref, cos_ref, sin_ref, mask_ref, out_ref, acc_ref):
    step = pl.program_id(0)

    @pl.when(step == 0)
    def _():
        acc_ref[...] = jnp.zeros_like(acc_ref)

    for n, w_ref in enumerate((w0_ref, w1_ref, w2_ref)):
        total = acc_ref[:, n * 256 : n * 256 + 256]
        for zl in range(NZL):
            rows = w_ref[0, :, 0, :, zl].reshape(NX * NZH * ROWS, 256)
            total += jnp.dot(x_ref[:, zl * 256 : zl * 256 + 256], rows, preferred_element_type=jnp.float32)
        acc_ref[:, n * 256 : n * 256 + 256] = total

    @pl.when(step == pl.num_programs(0) - 1)
    def _():
        inv, cos, sin = inv_ref[...], cos_ref[...], sin_ref[...]
        allowed = mask_ref[...] > 0
        keys = rope(acc_ref[:, 512:640] * inv, cos, sin).astype(jnp.bfloat16)
        values = (acc_ref[:, 640:768] * inv).astype(jnp.bfloat16)
        for h in range(4):
            q = rope(acc_ref[:, h * HD : h * HD + HD] * inv, cos, sin).astype(jnp.bfloat16)
            s = lax.dot_general(q, keys, (((1,), (1,)), ((), ())), preferred_element_type=jnp.float32)
            s = jnp.where(allowed, s * (1.0 / math.sqrt(HD)), -1e30)
            e = jnp.exp(s - jnp.max(s, -1, keepdims=True))
            probs = (e / jnp.sum(e, -1, keepdims=True)).astype(jnp.bfloat16)
            out_ref[:, h * HD : h * HD + HD] = jnp.dot(
                probs, values, preferred_element_type=jnp.float32
            ).astype(jnp.bfloat16)


def project_kernel(mixed_ref, x_ref, w3_ref, w4_ref, out_ref):
    for zl in range(NZL):
        total = x_ref[:, zl * 256 : zl * 256 + 256].astype(jnp.float32)
        for n, w_ref in enumerate((w3_ref, w4_ref)):
            rows = w_ref[0, :, 0, :, zl].reshape(NX * NZH * ROWS, 256)
            total += lax.dot_general(
                mixed_ref[:, n * 256 : n * 256 + 256],
                rows,
                (((1,), (1,)), ((), ())),
                preferred_element_type=jnp.float32,
            )
        out_ref[:, zl * 256 : zl * 256 + 256] = total.astype(jnp.bfloat16)


def weight_spec(col):
    return pl.BlockSpec(
        (1, NX, 1, NZH, NZL, ROWS, 256), lambda s: (s // NC, 0, s % NC, 0, 0, 0, col)
    )


def body(stream, segment_ids, positions, norm_gain, q_weight, k_weight, v_weight, o_weight):
    gain = norm_gain[0].astype(jnp.float32)[:, None]
    qkv = jnp.concatenate([q_weight[0], k_weight[0], v_weight[0]], -1)
    qkv = (qkv.astype(jnp.float32) * gain).astype(jnp.bfloat16)
    local = jnp.concatenate([qkv, o_weight[0].T], -1)
    column = lax.all_gather(local, ("zh", "zl"), axis=0, tiled=True)
    whole = lax.all_gather(column, ("y", "x", "c"), axis=0, tiled=True)
    whole = whole.reshape(NY, NX, NC, NZH, NZL, ROWS, 1280)

    wide = stream.astype(jnp.float32)
    inv = lax.rsqrt(jnp.mean(wide * wide, -1, keepdims=True) + 1e-05)
    freqs = jnp.exp(-math.log(500000.0) * jnp.arange(HD // 2, dtype=jnp.float32) * 2.0 / HD)
    angles = positions.astype(jnp.float32)[:, None] * freqs[None, :]
    cos, sin = jnp.cos(angles), jnp.sin(angles)
    cos = jnp.concatenate([cos, cos], -1)
    sin = jnp.concatenate([-sin, sin], -1)
    allowed = (segment_ids[:, None] == segment_ids[None, :]) & (positions[None, :] <= positions[:, None])
    mask = allowed.astype(jnp.float32)

    steps = NY * NC
    whole_block = lambda shape: pl.BlockSpec(shape, lambda s: (0, 0))
    mixed = pl.pallas_call(
        attend_kernel,
        grid=(steps,),
        in_specs=[
            pl.BlockSpec((T, 1024), lambda s: (0, s)),
            weight_spec(0),
            weight_spec(1),
            weight_spec(2),
            whole_block((T, 1)),
            whole_block((T, HD)),
            whole_block((T, HD)),
            whole_block((T, T)),
        ],
        out_specs=whole_block((T, 512)),
        out_shape=jax.ShapeDtypeStruct((T, 512), jnp.bfloat16),
        scratch_shapes=[pltpu.VMEM((T, 768), jnp.float32)],
        compiler_params=pltpu.CompilerParams(dimension_semantics=("arbitrary",)),
        name="attend",
    )(stream, whole, whole, whole, inv, cos, sin, mask)
    return pl.pallas_call(
        project_kernel,
        grid=(steps,),
        in_specs=[
            whole_block((T, 512)),
            pl.BlockSpec((T, 1024), lambda s: (0, s)),
            weight_spec(3),
            weight_spec(4),
        ],
        out_specs=pl.BlockSpec((T, 1024), lambda s: (0, s)),
        out_shape=jax.ShapeDtypeStruct((T, 8192), jnp.bfloat16),
        compiler_params=pltpu.CompilerParams(dimension_semantics=("arbitrary",)),
        name="project",
    )(mixed, stream, whole, whole)


def solution(mesh):
    fine = Mesh(mesh.devices.reshape(NY, NC, NZL, NX, NZH), AXES)
    in_specs = (
        P(AXES, None),
        P(AXES),
        P(AXES),
        P(None, AXES),
        P(None, AXES, None),
        P(None, AXES, None),
        P(None, AXES, None),
        P(None, None, AXES),
    )
    return jax.shard_map(body, mesh=fine, in_specs=in_specs, out_specs=P(AXES, None), check_vma=False)
```

```python
import math

import jax
import jax.numpy as jnp
from jax import lax
from jax.experimental import pallas as pl
from jax.experimental.pallas import tpu as pltpu
from jax.sharding import Mesh, PartitionSpec as P


AXES = ("y", "c", "zl", "x", "zh")
NY, NC, NZL, NX, NZH = 4, 2, 4, 4, 2
RING = {"x": (("c", "x"), 4), "y": (("y", "c"), 4), "z": (("c", "zl", "zh"), 8)}
HD = 128
ROWS = 32
T = 256


def position(axis):
    if axis == "z":
        return lax.axis_index("zh") * NZL + lax.axis_index("zl")
    return lax.axis_index(axis)


def exchange(block, axis, step):
    names, n = RING[axis]

    def number(p, c):
        if axis == "z":
            return (c * NZL + p % NZL) * NZH + p // NZL
        return c * n + p if axis == "x" else p * NC + c

    pairs = []
    for p in range(n):
        for c in range(NC):
            right = ((p + c) % 2 == 0) == (step % 2 == 0)
            pairs.append((number(p, c), number((p + (1 if right else -1)) % n, c)))
    return lax.ppermute(block, names, pairs)


def gather(block, axis):
    n = RING[axis][1]
    other = exchange(block, axis, 0)
    first = (position(axis) + lax.axis_index("c")) % 2 == 0
    current = jnp.where(first, jnp.stack([block, other]), jnp.stack([other, block]))
    found = [current]
    for step in range(1, n // 2):
        current = exchange(current, axis, step)
        found.append(current)
    return found


def slots(axis, core):
    n = RING[axis][1]
    k = lax.iota(jnp.int32, n)
    p = position(axis)
    left = (p + core) & 1
    off = jnp.where((k >> 1) & 1 == 1, -((k >> 1) + 1), k >> 1 & -2)
    return (p - left + (1 - 2 * left) * off + (k & 1)) & (n - 1)


def table(core):
    return jnp.concatenate([slots("z", core), slots("x", core), slots("y", core)]).astype(jnp.int32)


def rope(h, cos, sin):
    return h * cos + pltpu.roll(h, HD // 2, 1) * sin


def qkv_kernel(tab, x_ref, xp_ref, a0_ref, a1_ref, b0_ref, b1_ref, own_ref, par_ref, xs, wa, wb, sem):
    core = tab[16]
    for y in range(NY):
        pltpu.make_async_copy(
            x_ref.at[:, pl.ds(y * 2048 + core * 1024, 1024)], xs.at[0, :, pl.ds(y * 1024, 1024)], sem.at[0]
        ).start()
    pltpu.make_async_copy(xp_ref, xs.at[1], sem.at[0]).start()

    def place(k, _):
        z = tab[k]
        zh, zl = z // NZL, z % NZL
        for half in range(2):
            a_ref, b_ref = ((a0_ref, b0_ref), (a1_ref, b1_ref))[half]
            for i in range(2):
                for j in range(4):
                    outer, inner = half * 2 + i, j
                    pltpu.make_async_copy(
                        a_ref.at[i, j, k], wa.at[tab[12 + outer], zl, tab[8 + inner], zh], sem.at[1]
                    ).start()
                    pltpu.make_async_copy(
                        b_ref.at[i, j, k], wb.at[tab[12 + inner], zl, tab[8 + outer], zh], sem.at[2]
                    ).start()
        return 0

    lax.fori_loop(0, 8, place, 0)
    pltpu.make_async_copy(xs, xs, sem.at[0]).wait()
    for col, w, s in ((0, wa, 1), (384, wb, 2)):
        pltpu.make_async_copy(w, w, sem.at[s]).wait()
        rows = w[...].reshape(4096, 384)
        par_ref[:, col : col + 384] = jnp.dot(xs[1], rows, preferred_element_type=jnp.float32)
        own_ref[:, col : col + 384] = jnp.dot(xs[0], rows, preferred_element_type=jnp.float32)


def finish_kernel(
    tab, tab_par, own_ref, par_ref, inv_ref, cos_ref, sin_ref, mask_ref, x_ref,
    o0, o1, o2, o3, p0, p1, p2, p3, out_ref, ot, xs, ys, mixed, sem, ysem,
):
    pltpu.make_async_copy(x_ref, xs, sem.at[0]).start()
    core = tab[16]
    for t, pieces, c in ((tab, (o0, o1, o2, o3), core), (tab_par, (p0, p1, p2, p3), 1 - core)):

        def place(k, _, t=t, pieces=pieces, c=c):
            y, x = t[12 + k // NX], t[8 + k % NX]
            for n, piece in enumerate(pieces):
                for i in range(2):
                    z = t[n * 2 + i]
                    pltpu.make_async_copy(
                        piece.at[i, k // NX, k % NX], ot.at[y, c, z % NZL, x, z // NZL], sem.at[1]
                    ).start()
            return 0

        lax.fori_loop(0, NY * NX, place, 0)

    inv, cos, sin = inv_ref[...], cos_ref[...], sin_ref[...]
    allowed = mask_ref[...] > 0

    def raw(col):
        return (own_ref[:, col : col + HD] + par_ref[:, col : col + HD]) * inv

    keys = rope(raw(512), cos, sin).astype(jnp.bfloat16)
    values = raw(640).astype(jnp.bfloat16)
    for h in range(4):
        q = rope(raw(h * HD), cos, sin).astype(jnp.bfloat16)
        s = lax.dot_general(q, keys, (((1,), (1,)), ((), ())), preferred_element_type=jnp.float32)
        s = jnp.where(allowed, s * (1.0 / math.sqrt(HD)), -1e30)
        e = jnp.exp(s - jnp.max(s, -1, keepdims=True))
        probs = (e / jnp.sum(e, -1, keepdims=True)).astype(jnp.bfloat16)
        mixed[:, h * HD : h * HD + HD] = jnp.dot(
            probs, values, preferred_element_type=jnp.float32
        ).astype(jnp.bfloat16)
    pltpu.make_async_copy(xs, xs, sem.at[0]).wait()
    pltpu.make_async_copy(ot, ot, sem.at[1]).wait()
    writes = []
    for k in range(NY * NC):
        rows = ot[k // NC, k % NC].reshape(1024, 512)
        branch = lax.dot_general(
            mixed[...], rows, (((1,), (1,)), ((), ())), preferred_element_type=jnp.float32
        )
        ys[k] = (xs[:, k * 1024 : k * 1024 + 1024].astype(jnp.float32) + branch).astype(jnp.bfloat16)
        writes.append(pltpu.make_async_copy(ys.at[k], out_ref.at[:, pl.ds(k * 1024, 1024)], ysem.at[k]))
        writes[-1].start()
    for w in writes:
        w.wait()


def body(stream, segment_ids, positions, norm_gain, q_weight, k_weight, v_weight, o_weight):
    core = lax.axis_index("c")
    swap = lambda a: lax.ppermute(a, "c", [(0, 1), (1, 0)])
    gain = norm_gain[0].astype(jnp.float32)[:, None]
    qkv = jnp.concatenate([q_weight[0], k_weight[0], v_weight[0]], -1)
    qkv = (qkv.astype(jnp.float32) * gain).astype(jnp.bfloat16)

    column = jnp.concatenate(gather(qkv, "z"))
    a, b = column[:, :, :384], column[:, :, 384:]
    a = jnp.concatenate(gather(a, "x"))
    b = jnp.concatenate(gather(b, "y"))
    a = gather(a, "y")
    b = gather(b, "x")

    o = jnp.concatenate(gather(o_weight[0].T, "x"))
    o = jnp.concatenate(gather(o, "y"))
    o = gather(o, "z")
    o_par = [swap(v) for v in o]

    half = lambda c: jnp.concatenate([stream[:, (2 * y + c) * 1024 :][:, :1024] for y in range(NY)], 1)
    x_par = swap(jnp.where(core == 0, half(1), half(0)))

    wide = stream.astype(jnp.float32)
    inv = lax.rsqrt(jnp.mean(wide * wide, -1, keepdims=True) + 1e-05)
    freqs = jnp.exp(-math.log(500000.0) * jnp.arange(HD // 2, dtype=jnp.float32) * 2.0 / HD)
    angles = positions.astype(jnp.float32)[:, None] * freqs[None, :]
    cos, sin = jnp.cos(angles), jnp.sin(angles)
    cos = jnp.concatenate([cos, cos], -1)
    sin = jnp.concatenate([-sin, sin], -1)
    allowed = (segment_ids[:, None] == segment_ids[None, :]) & (positions[None, :] <= positions[:, None])
    mask = allowed.astype(jnp.float32)

    tab = jnp.concatenate([table(core), core[None].astype(jnp.int32)])
    tab_par = table(1 - core)

    smem = pl.BlockSpec(memory_space=pltpu.SMEM)
    vmem = pl.BlockSpec(memory_space=pltpu.VMEM)
    hbm = pl.BlockSpec(memory_space=pl.ANY)
    partial = jax.ShapeDtypeStruct((T, 768), jnp.float32)
    own, par = pl.pallas_call(
        qkv_kernel,
        in_specs=[smem] + [hbm] * 6,
        out_specs=[vmem, vmem],
        out_shape=[partial, partial],
        scratch_shapes=[
            pltpu.VMEM((2, T, 4096), jnp.bfloat16),
            pltpu.VMEM((NY, NZL, NX, NZH, ROWS, 384), jnp.bfloat16),
            pltpu.VMEM((NY, NZL, NX, NZH, ROWS, 384), jnp.bfloat16),
            pltpu.SemaphoreType.DMA((3,)),
        ],
        name="qkv",
    )(tab, stream, x_par, *a, *b)
    par = swap(par)
    return pl.pallas_call(
        finish_kernel,
        in_specs=[smem, smem] + [vmem] * 6 + [hbm] * 9,
        out_specs=hbm,
        out_shape=jax.ShapeDtypeStruct((T, 8192), jnp.bfloat16),
        scratch_shapes=[
            pltpu.VMEM((NY, NC, NZL, NX, NZH, ROWS, 512), jnp.bfloat16),
            pltpu.VMEM((T, 8192), jnp.bfloat16),
            pltpu.VMEM((NY * NC, T, 1024), jnp.bfloat16),
            pltpu.VMEM((T, 512), jnp.bfloat16),
            pltpu.SemaphoreType.DMA((2,)),
            pltpu.SemaphoreType.DMA((NY * NC,)),
        ],
        name="finish",
    )(tab, tab_par, own, par, inv, cos, sin, mask, stream, *o, *o_par)


def solution(mesh):
    fine = Mesh(mesh.devices.reshape(NY, NC, NZL, NX, NZH), AXES)
    in_specs = (
        P(AXES, None),
        P(AXES),
        P(AXES),
        P(None, AXES),
        P(None, AXES, None),
        P(None, AXES, None),
        P(None, AXES, None),
        P(None, None, AXES),
    )
    return jax.shard_map(body, mesh=fine, in_specs=in_specs, out_specs=P(AXES, None), check_vma=False)
```

```python
import functools
import math

import jax
import jax.numpy as jnp
from jax import lax
from jax.experimental import pallas as pl
from jax.experimental.pallas import tpu as pltpu
from jax.sharding import Mesh, PartitionSpec as P


AXES = ("y", "c", "zl", "x", "zh")
NY, NC, NZL, NX, NZH = 4, 2, 4, 4, 2
RING = {"x": (("c", "x"), 4), "y": (("y", "c"), 4), "z": (("c", "zl", "zh"), 8)}
HD = 128
ROWS = 32
T = 256


def position(axis):
    if axis == "z":
        return lax.axis_index("zh") * NZL + lax.axis_index("zl")
    return lax.axis_index(axis)


def exchange(block, axis, step):
    names, n = RING[axis]

    def number(p, c):
        if axis == "z":
            return (c * NZL + p % NZL) * NZH + p // NZL
        return c * n + p if axis == "x" else p * NC + c

    pairs = []
    for p in range(n):
        for c in range(NC):
            right = ((p + c) % 2 == 0) == (step % 2 == 0)
            pairs.append((number(p, c), number((p + (1 if right else -1)) % n, c)))
    return lax.ppermute(block, names, pairs)


def gather(block, axis):
    n = RING[axis][1]
    other = exchange(block, axis, 0)
    first = (position(axis) + lax.axis_index("c")) % 2 == 0
    current = jnp.where(first, jnp.stack([block, other]), jnp.stack([other, block]))
    found = [current]
    for step in range(1, n // 2):
        current = exchange(current, axis, step)
        found.append(current)
    return found


def slots(axis, core):
    n = RING[axis][1]
    k = lax.iota(jnp.int32, n)
    p = position(axis)
    left = (p + core) & 1
    off = jnp.where((k >> 1) & 1 == 1, -((k >> 1) + 1), k >> 1 & -2)
    return (p - left + (1 - 2 * left) * off + (k & 1)) & (n - 1)


def near(axis, core):
    k = lax.iota(jnp.int32, 4)
    p = position(axis)
    turn = 1 - 2 * ((p + core) & 1)
    return (p + turn * jnp.where(k == 2, -1, k) + jnp.where(k == 3, -turn, 0)) & 3


def spread(block, axis):
    one = exchange(block, axis, 0)
    two = exchange(block, axis, 1)
    return [block, one, two, exchange(one, axis, 1)]


Z, ZP, X, Y, XO, YO, CORE = 0, 8, 16, 20, 24, 28, 32


def table():
    core = lax.axis_index("c")
    parts = [slots("z", core), slots("z", 1 - core), near("x", core), near("y", core)]
    parts += [slots("x", core), slots("y", core), core[None]]
    return jnp.concatenate(parts).astype(jnp.int32)


def arrange_columns_kernel(tab, p0, p1, p2, p3, a_ref, b_ref):
    for n, p in enumerate((p0, p1, p2, p3)):
        for i in range(2):
            z = tab[Z + n * 2 + i]
            a_ref[z % NZL, z // NZL] = p[i, :, :384]
            b_ref[z % NZL, z // NZL] = p[i, :, 384:]


def arrange_kernel(at, tab, p0, p1, p2, p3, out_ref):
    for n, p in enumerate((p0, p1, p2, p3)):
        out_ref[tab[at + n]] = p[...]


def arrange_plane_kernel(tab, p0, p1, out_ref):
    for n, p in enumerate((p0, p1)):
        for i in range(2):
            for j in range(4):
                out_ref[tab[YO + n * 2 + i], tab[XO + j]] = p[i, j]


def local(kernel, tab, arrays, shapes):
    vmem = pl.BlockSpec(memory_space=pltpu.VMEM)
    out = [jax.ShapeDtypeStruct(s, jnp.bfloat16) for s in shapes]
    return pl.pallas_call(
        kernel,
        in_specs=[pl.BlockSpec(memory_space=pltpu.SMEM)] + [vmem] * len(arrays),
        out_specs=[vmem] * len(out),
        out_shape=out,
    )(tab, *arrays)


def rope(h, cos, sin):
    return h * cos + pltpu.roll(h, HD // 2, 1) * sin


def other_half_kernel(tab, x_ref, out_ref, sem):
    copies = [
        pltpu.make_async_copy(
            x_ref.at[:, pl.ds(y * 2048 + (1 - tab[CORE]) * 1024, 1024)],
            out_ref.at[:, pl.ds(y * 1024, 1024)],
            sem.at[y],
        )
        for y in range(NY)
    ]
    for c in copies:
        c.start()
    for c in copies:
        c.wait()


def token_copies(tab, x_ref, xp_ref, y, dst, sems):
    return [
        pltpu.make_async_copy(
            x_ref.at[:, pl.ds(pl.multiple_of(y * 2048 + tab[CORE] * 1024, 1024), 1024)], dst.at[pl.ds(0, T)], sems[0]
        ),
        pltpu.make_async_copy(
            xp_ref.at[:, pl.ds(pl.multiple_of(y * 1024, 1024), 1024)], dst.at[pl.ds(T, T)], sems[1]
        ),
    ]


def prepare_kernel(tab, x_ref, xp_ref, xb_ref, ps, sem):
    copies = [token_copies(tab, x_ref, xp_ref, y, ps.at[y], (sem.at[y], sem.at[4 + y])) for y in range(NY)]
    for pair in copies:
        for c in pair:
            c.start()
    low = lax.broadcasted_iota(jnp.int32, (2 * T, 128), 1) < 64
    for y in range(NY):
        for c in copies[y]:
            c.wait()
        for zl in range(0, NZL, 2):
            for x in range(NX):
                at = zl * 256 + x // 2 * 128
                one = ps[y, :, at : at + 128].astype(jnp.float32)
                two = ps[y, :, at + 256 : at + 384].astype(jnp.float32)
                if x % 2 == 0:
                    both = jnp.where(low, one, pltpu.roll(two, 64, 1))
                else:
                    both = jnp.where(low, pltpu.roll(one, 64, 1), two)
                xb_ref[x, :, y * 256 + zl * 64 : y * 256 + zl * 64 + 128] = both.astype(jnp.bfloat16)


def product(colour, slot, count, tab, x_refs, w_refs, x, w, sem):
    x_ref, xp_ref, xb_ref = x_refs
    waits = []
    for i in range(count):
        if colour == "a":
            group = token_copies(tab, x_ref, xp_ref, tab[Y + slot + i], x.at[i], (sem.at[3 * i], sem.at[3 * i + 1]))
            blocks = [pltpu.make_async_copy(w_refs[i].at[j], w.at[i, :, j], sem.at[3 * i + 2]) for j in range(NX)]
        else:
            group = [pltpu.make_async_copy(xb_ref.at[tab[X + slot + i]], x.at[i], sem.at[3 * i])]
            blocks = [pltpu.make_async_copy(w_refs[i], w.at[i], sem.at[3 * i + 2])]
        for c in group + blocks:
            c.start()
        waits.append(group + [pltpu.make_async_copy(w.at[i], w.at[i], sem.at[3 * i + 2])])

    def finish():
        total = None
        for i in range(count):
            for c in waits[i]:
                c.wait()
            part = jnp.dot(x[i], w[i].reshape(1024, 384), preferred_element_type=jnp.float32)
            total = part if total is None else total + part
        return total

    return finish


def first_kernel(colour, tab, x_ref, xp_ref, xb_ref, w0, w1, w2, out_ref, x, w, sem):
    out_ref[...] = product(colour, 0, 3, tab, (x_ref, xp_ref, xb_ref), (w0, w1, w2), x, w, sem)()


def last_kernel(tab, x_ref, xp_ref, xb_ref, a, b, ta_ref, tb_ref, own_ref, par_ref, x, wa, wb, t, sem, tsem):
    x_refs = (x_ref, xp_ref, xb_ref)
    finish = [product("a", 3, 1, tab, x_refs, (a,), x.at[pl.ds(0, 1)], wa, sem.at[pl.ds(0, 3)])]
    finish.append(product("b", 3, 1, tab, x_refs, (b,), x.at[pl.ds(1, 1)], wb, sem.at[pl.ds(3, 3)]))
    before = [pltpu.make_async_copy(r, t.at[n], tsem.at[n]) for n, r in enumerate((ta_ref, tb_ref))]
    for c in before:
        c.start()
    for n in range(2):
        total = finish[n]()
        before[n].wait()
        total += t[n]
        own_ref[:, n * 384 : n * 384 + 384] = total[:T]
        par_ref[:, n * 384 : n * 384 + 384] = total[T:]


WEIGHTS = {"a": (NZL, NX, NZH, ROWS, 384), "b": (NY, NZL, NZH, ROWS, 384)}


def first_products(colour, tab, xs, w):
    hbm = pl.BlockSpec(memory_space=pl.ANY)
    return pl.pallas_call(
        functools.partial(first_kernel, colour),
        in_specs=[pl.BlockSpec(memory_space=pltpu.SMEM)] + [hbm] * 6,
        out_specs=pl.BlockSpec(memory_space=pltpu.VMEM),
        out_shape=jax.ShapeDtypeStruct((2 * T, 384), jnp.float32),
        scratch_shapes=[
            pltpu.VMEM((3, 2 * T, 1024), jnp.bfloat16),
            pltpu.VMEM((3, *WEIGHTS[colour]), jnp.bfloat16),
            pltpu.SemaphoreType.DMA((9,)),
        ],
    )(tab, *xs, *w)


def last_products(tab, xs, a, b, ta, tb):
    hbm = pl.BlockSpec(memory_space=pl.ANY)
    return pl.pallas_call(
        last_kernel,
        in_specs=[pl.BlockSpec(memory_space=pltpu.SMEM)] + [hbm] * 7,
        out_specs=[pl.BlockSpec(memory_space=pltpu.VMEM)] * 2,
        out_shape=[jax.ShapeDtypeStruct((T, 768), jnp.float32)] * 2,
        scratch_shapes=[
            pltpu.VMEM((2, 2 * T, 1024), jnp.bfloat16),
            pltpu.VMEM((1, *WEIGHTS["a"]), jnp.bfloat16),
            pltpu.VMEM((1, *WEIGHTS["b"]), jnp.bfloat16),
            pltpu.VMEM((2, 2 * T, 384), jnp.float32),
            pltpu.SemaphoreType.DMA((6,)),
            pltpu.SemaphoreType.DMA((2,)),
        ],
        name="last",
    )(tab, *xs, a, b, ta, tb)


def finish_kernel(
    tab, own_ref, par_ref, inv_ref, cos_ref, sin_ref, mask_ref, x_ref,
    o0, o1, o2, o3, p0, p1, p2, p3, out_ref, ot, xs, ys, mixed, sem, ysem,
):
    pltpu.make_async_copy(x_ref, xs, sem.at[0]).start()
    core = tab[CORE]
    for at, pieces, c in ((Z, (o0, o1, o2, o3), core), (ZP, (p0, p1, p2, p3), 1 - core)):
        for n, piece in enumerate(pieces):
            for i in range(2):
                z = tab[at + n * 2 + i]
                for y in range(NY):
                    pltpu.make_async_copy(
                        piece.at[i, y], ot.at[y, c, z % NZL, :, z // NZL], sem.at[1]
                    ).start()
    inv, cos, sin = inv_ref[...], cos_ref[...], sin_ref[...]
    allowed = mask_ref[...] > 0

    def raw(col):
        return (own_ref[:, col : col + HD] + par_ref[:, col : col + HD]) * inv

    keys = rope(raw(512), cos, sin).astype(jnp.bfloat16)
    values = raw(640).astype(jnp.bfloat16)
    for h in range(4):
        q = rope(raw(h * HD), cos, sin).astype(jnp.bfloat16)
        s = lax.dot_general(q, keys, (((1,), (1,)), ((), ())), preferred_element_type=jnp.float32)
        s = jnp.where(allowed, s * (1.0 / math.sqrt(HD)), -1e30)
        e = jnp.exp(s - jnp.max(s, -1, keepdims=True))
        probs = (e / jnp.sum(e, -1, keepdims=True)).astype(jnp.bfloat16)
        mixed[:, h * HD : h * HD + HD] = jnp.dot(
            probs, values, preferred_element_type=jnp.float32
        ).astype(jnp.bfloat16)
    pltpu.make_async_copy(xs, xs, sem.at[0]).wait()
    pltpu.make_async_copy(ot, ot, sem.at[1]).wait()
    writes = []
    for k in range(NY * NC):
        rows = ot[k // NC, k % NC].reshape(1024, 512)
        branch = lax.dot_general(
            mixed[...], rows, (((1,), (1,)), ((), ())), preferred_element_type=jnp.float32
        )
        ys[k] = (xs[:, k * 1024 : k * 1024 + 1024].astype(jnp.float32) + branch).astype(jnp.bfloat16)
        writes.append(pltpu.make_async_copy(ys.at[k], out_ref.at[:, pl.ds(k * 1024, 1024)], ysem.at[k]))
        writes[-1].start()
    for w in writes:
        w.wait()


def body(stream, segment_ids, positions, norm_gain, q_weight, k_weight, v_weight, o_weight):
    gain = norm_gain[0].astype(jnp.float32)[:, None]
    qkv = jnp.concatenate([q_weight[0], k_weight[0], v_weight[0]], -1)
    qkv = lax.optimization_barrier((qkv.astype(jnp.float32) * gain).astype(jnp.bfloat16))

    tab = table()
    smem = pl.BlockSpec(memory_space=pltpu.SMEM)
    vmem = pl.BlockSpec(memory_space=pltpu.VMEM)
    hbm = pl.BlockSpec(memory_space=pl.ANY)

    shape = (NZL, NZH, ROWS, 384)
    a, b = local(arrange_columns_kernel, tab, gather(qkv, "z"), [shape] * 2)
    a, b = spread(a, "x"), spread(b, "y")
    (a,) = local(functools.partial(arrange_kernel, X), tab, a, [(NX, *shape)])
    (b,) = local(functools.partial(arrange_kernel, Y), tab, b, [(NY, *shape)])
    a, b = spread(a, "y"), spread(b, "x")

    o, _ = lax.optimization_barrier((o_weight[0].T, qkv))
    o = jnp.concatenate(gather(o, "x"))
    (o,) = local(arrange_plane_kernel, tab, gather(o, "y"), [(NY, NX, ROWS, 512)])
    o = gather(o, "z")

    def swap(a):
        return lax.ppermute(a, "c", [(0, 1), (1, 0)])

    o_par = [swap(v) for v in o]

    freqs = jnp.exp(-math.log(500000.0) * jnp.arange(HD // 2, dtype=jnp.float32) * 2.0 / HD)
    angles = positions.astype(jnp.float32)[:, None] * freqs[None, :]
    cos, sin = jnp.cos(angles), jnp.sin(angles)
    cos = jnp.concatenate([cos, cos], -1)
    sin = jnp.concatenate([-sin, sin], -1)
    allowed = (segment_ids[:, None] == segment_ids[None, :]) & (positions[None, :] <= positions[:, None])
    mask = allowed.astype(jnp.float32)

    x_par = pl.pallas_call(
        other_half_kernel,
        in_specs=[smem, hbm],
        out_specs=vmem,
        out_shape=jax.ShapeDtypeStruct((T, 4096), jnp.bfloat16),
        scratch_shapes=[pltpu.SemaphoreType.DMA((NY,))],
        name="other_half",
    )(tab, stream)
    x_par = swap(x_par)
    x_cut = pl.pallas_call(
        prepare_kernel,
        in_specs=[smem, hbm, hbm],
        out_specs=vmem,
        out_shape=jax.ShapeDtypeStruct((4, 2 * T, 1024), jnp.bfloat16),
        scratch_shapes=[
            pltpu.VMEM((4, 2 * T, 1024), jnp.bfloat16),
            pltpu.SemaphoreType.DMA((8,)),
        ],
        name="prepare",
    )(tab, stream, x_par)
    wide = stream.astype(jnp.float32)
    inv = lax.rsqrt(jnp.mean(wide * wide, -1, keepdims=True) + 1e-05)
    xs = (stream, x_par, x_cut)
    total_a = first_products("a", tab, xs, a[:3])
    total_b = first_products("b", tab, xs, b[:3])
    own, par = last_products(tab, xs, a[3], b[3], total_a, total_b)
    par = swap(par)
    return pl.pallas_call(
        finish_kernel,
        in_specs=[smem] + [vmem] * 6 + [hbm] * 9,
        out_specs=hbm,
        out_shape=jax.ShapeDtypeStruct((T, 8192), jnp.bfloat16),
        scratch_shapes=[
            pltpu.VMEM((NY, NC, NZL, NX, NZH, ROWS, 512), jnp.bfloat16),
            pltpu.VMEM((T, 8192), jnp.bfloat16),
            pltpu.VMEM((NY * NC, T, 1024), jnp.bfloat16),
            pltpu.VMEM((T, 512), jnp.bfloat16),
            pltpu.SemaphoreType.DMA((2,)),
            pltpu.SemaphoreType.DMA((NY * NC,)),
        ],
        name="finish",
    )(tab, own, par, inv, cos, sin, mask, stream, *o, *o_par)


def solution(mesh):
    fine = Mesh(mesh.devices.reshape(NY, NC, NZL, NX, NZH), AXES)
    in_specs = (
        P(AXES, None),
        P(AXES),
        P(AXES),
        P(None, AXES),
        P(None, AXES, None),
        P(None, AXES, None),
        P(None, AXES, None),
        P(None, None, AXES),
    )

    return jax.shard_map(body, mesh=fine, in_specs=in_specs, out_specs=P(AXES, None), check_vma=False)
```

```python
import functools
import math

import jax
import jax.numpy as jnp
from jax import lax
from jax.experimental import pallas as pl
from jax.experimental.pallas import tpu as pltpu
from jax.sharding import Mesh, PartitionSpec as P


AXES = ("y", "c", "zl", "x", "zh")
NY, NC, NZL, NX, NZH = 4, 2, 4, 4, 2
RING = {"x": (("c", "x"), 4), "y": (("y", "c"), 4), "z": (("c", "zl", "zh"), 8)}
VMEM_LIMIT = pltpu.CompilerParams(vmem_limit_bytes=20 * 1024 * 1024)
HD = 128
ROWS = 32
T = 256


def position(axis):
    if axis == "z":
        return lax.axis_index("zh") * NZL + lax.axis_index("zl")
    return lax.axis_index(axis)


def exchange(block, axis, step):
    names, n = RING[axis]

    def number(p, c):
        if axis == "z":
            return (c * NZL + p % NZL) * NZH + p // NZL
        return c * n + p if axis == "x" else p * NC + c

    pairs = []
    for p in range(n):
        for c in range(NC):
            right = ((p + c) % 2 == 0) == (step % 2 == 0)
            pairs.append((number(p, c), number((p + (1 if right else -1)) % n, c)))
    return lax.ppermute(block, names, pairs)


def gather(block, axis):
    n = RING[axis][1]
    other = exchange(block, axis, 0)
    first = (position(axis) + lax.axis_index("c")) % 2 == 0
    current = jnp.where(first, jnp.stack([block, other]), jnp.stack([other, block]))
    found = [current]
    for step in range(1, n // 2):
        current = exchange(current, axis, step)
        found.append(current)
    return found


def slots(axis, core):
    n = RING[axis][1]
    k = lax.iota(jnp.int32, n)
    p = position(axis)
    left = (p + core) & 1
    off = jnp.where((k >> 1) & 1 == 1, -((k >> 1) + 1), k >> 1 & -2)
    return (p - left + (1 - 2 * left) * off + (k & 1)) & (n - 1)


def near(axis, core):
    k = lax.iota(jnp.int32, 4)
    p = position(axis)
    turn = 1 - 2 * ((p + core) & 1)
    return (p + turn * jnp.where(k == 2, -1, k) + jnp.where(k == 3, -turn, 0)) & 3


def spread(block, axis):
    one = exchange(block, axis, 0)
    two = exchange(block, axis, 1)
    return [block, one, two, exchange(one, axis, 1)]


Z, ZP, X, Y, XO, YO, CORE = 0, 8, 16, 20, 24, 28, 32


def table():
    core = lax.axis_index("c")
    parts = [slots("z", core), slots("z", 1 - core), near("x", core), near("y", core)]
    parts += [slots("x", core), slots("y", core), core[None]]
    return jnp.concatenate(parts).astype(jnp.int32)


def arrange_columns_kernel(tab, p0, p1, p2, p3, a_ref, b_ref):
    for n, p in enumerate((p0, p1, p2, p3)):
        for i in range(2):
            z = tab[Z + n * 2 + i]
            a_ref[z % NZL, z // NZL] = p[i, :, :384]
            b_ref[z % NZL, z // NZL] = p[i, :, 384:]


def arrange_kernel(at, tab, p0, p1, p2, p3, out_ref):
    for n, p in enumerate((p0, p1, p2, p3)):
        out_ref[tab[at + n]] = p[...]


def arrange_plane_kernel(tab, p0, p1, out_ref):
    for n, p in enumerate((p0, p1)):
        for i in range(2):
            for j in range(4):
                out_ref[tab[YO + n * 2 + i], tab[XO + j]] = p[i, j]


def local(kernel, tab, arrays, shapes):
    vmem = pl.BlockSpec(memory_space=pltpu.VMEM)
    out = [jax.ShapeDtypeStruct(s, jnp.bfloat16) for s in shapes]
    return pl.pallas_call(
        kernel,
        in_specs=[pl.BlockSpec(memory_space=pltpu.SMEM)] + [vmem] * len(arrays),
        out_specs=[vmem] * len(out),
        out_shape=out,
        compiler_params=VMEM_LIMIT,
    )(tab, *arrays)


def rope(h, cos, sin):
    return h * cos + pltpu.roll(h, HD // 2, 1) * sin


def other_half_kernel(tab, x_ref, out_ref, sem):
    copies = [
        pltpu.make_async_copy(
            x_ref.at[:, pl.ds(y * 2048 + (1 - tab[CORE]) * 1024, 1024)],
            out_ref.at[:, pl.ds(y * 1024, 1024)],
            sem.at[y],
        )
        for y in range(NY)
    ]
    for c in copies:
        c.start()
    for c in copies:
        c.wait()


def token_copies(tab, x_ref, xp_ref, y, dst, sems):
    return [
        pltpu.make_async_copy(
            x_ref.at[:, pl.ds(pl.multiple_of(y * 2048 + tab[CORE] * 1024, 1024), 1024)], dst.at[pl.ds(0, T)], sems[0]
        ),
        pltpu.make_async_copy(
            xp_ref.at[:, pl.ds(pl.multiple_of(y * 1024, 1024), 1024)], dst.at[pl.ds(T, T)], sems[1]
        ),
    ]


def rms_kernel(x_ref, kept_ref, inv_ref, sem):
    loads = [
        pltpu.make_async_copy(x_ref.at[:, pl.ds(k * 1024, 1024)], kept_ref.at[k], sem.at[k]) for k in range(8)
    ]
    for c in loads:
        c.start()
    total = jnp.zeros((T, 128), jnp.float32)
    for k, c in enumerate(loads):
        c.wait()
        for n in range(8):
            v = kept_ref[k, :, n * 128 : n * 128 + 128].astype(jnp.float32)
            total += v * v
    inv_ref[...] = lax.rsqrt(jnp.sum(total, -1, keepdims=True) * (1.0 / 8192) + 1e-05)


def prepare_kernel(tab, x_ref, xp_ref, xb_ref, ps, sem):
    copies = [token_copies(tab, x_ref, xp_ref, y, ps.at[y], (sem.at[y], sem.at[4 + y])) for y in range(NY)]
    for pair in copies:
        for c in pair:
            c.start()
    low = lax.broadcasted_iota(jnp.int32, (2 * T, 128), 1) < 64
    for y in range(NY):
        for c in copies[y]:
            c.wait()
        for zl in range(0, NZL, 2):
            for x in range(NX):
                at = zl * 256 + x // 2 * 128
                one = ps[y, :, at : at + 128].astype(jnp.float32)
                two = ps[y, :, at + 256 : at + 384].astype(jnp.float32)
                if x % 2 == 0:
                    both = jnp.where(low, one, pltpu.roll(two, 64, 1))
                else:
                    both = jnp.where(low, pltpu.roll(one, 64, 1), two)
                xb_ref[x, :, y * 256 + zl * 64 : y * 256 + zl * 64 + 128] = both.astype(jnp.bfloat16)


def product(colour, slot, count, tab, x_refs, w_refs, x, w, sem):
    x_ref, xp_ref, xb_ref = x_refs
    waits = []
    for i in range(count):
        if colour == "a":
            group = token_copies(tab, x_ref, xp_ref, tab[Y + slot + i], x.at[i], (sem.at[3 * i], sem.at[3 * i + 1]))
            blocks = [pltpu.make_async_copy(w_refs[i].at[j], w.at[i, :, j], sem.at[3 * i + 2]) for j in range(NX)]
        else:
            group = [pltpu.make_async_copy(xb_ref.at[tab[X + slot + i]], x.at[i], sem.at[3 * i])]
            blocks = [pltpu.make_async_copy(w_refs[i], w.at[i], sem.at[3 * i + 2])]
        for c in group + blocks:
            c.start()
        waits.append(group + [pltpu.make_async_copy(w.at[i], w.at[i], sem.at[3 * i + 2])])

    def finish():
        total = None
        for i in range(count):
            for c in waits[i]:
                c.wait()
            part = jnp.dot(x[i], w[i].reshape(1024, 384), preferred_element_type=jnp.float32)
            total = part if total is None else total + part
        return total

    return finish


def first_kernel(colour, tab, x_ref, xp_ref, xb_ref, w0, w1, w2, out_ref, x, w, sem):
    out_ref[...] = product(colour, 0, 3, tab, (x_ref, xp_ref, xb_ref), (w0, w1, w2), x, w, sem)()


def last_kernel(tab, x_ref, xp_ref, xb_ref, a, b, ta_ref, tb_ref, own_ref, par_ref, x, wa, wb, t, sem, tsem):
    x_refs = (x_ref, xp_ref, xb_ref)
    finish = [product("a", 3, 1, tab, x_refs, (a,), x.at[pl.ds(0, 1)], wa, sem.at[pl.ds(0, 3)])]
    finish.append(product("b", 3, 1, tab, x_refs, (b,), x.at[pl.ds(1, 1)], wb, sem.at[pl.ds(3, 3)]))
    before = [pltpu.make_async_copy(r, t.at[n], tsem.at[n]) for n, r in enumerate((ta_ref, tb_ref))]
    for c in before:
        c.start()
    for n in range(2):
        total = finish[n]()
        before[n].wait()
        total += t[n]
        own_ref[:, n * 384 : n * 384 + 384] = total[:T]
        par_ref[:, n * 384 : n * 384 + 384] = total[T:]


WEIGHTS = {"a": (NZL, NX, NZH, ROWS, 384), "b": (NY, NZL, NZH, ROWS, 384)}


def first_products(colour, tab, xs, w):
    hbm = pl.BlockSpec(memory_space=pl.ANY)
    return pl.pallas_call(
        functools.partial(first_kernel, colour),
        in_specs=[pl.BlockSpec(memory_space=pltpu.SMEM)] + [hbm] * 6,
        out_specs=pl.BlockSpec(memory_space=pltpu.VMEM),
        out_shape=jax.ShapeDtypeStruct((2 * T, 384), jnp.float32),
        scratch_shapes=[
            pltpu.VMEM((3, 2 * T, 1024), jnp.bfloat16),
            pltpu.VMEM((3, *WEIGHTS[colour]), jnp.bfloat16),
            pltpu.SemaphoreType.DMA((9,)),
        ],
        compiler_params=VMEM_LIMIT,
    )(tab, *xs, *w)


def last_products(tab, xs, a, b, ta, tb):
    hbm = pl.BlockSpec(memory_space=pl.ANY)
    return pl.pallas_call(
        last_kernel,
        in_specs=[pl.BlockSpec(memory_space=pltpu.SMEM)] + [hbm] * 7,
        out_specs=[pl.BlockSpec(memory_space=pltpu.VMEM)] * 2,
        out_shape=[jax.ShapeDtypeStruct((T, 768), jnp.float32)] * 2,
        scratch_shapes=[
            pltpu.VMEM((2, 2 * T, 1024), jnp.bfloat16),
            pltpu.VMEM((1, *WEIGHTS["a"]), jnp.bfloat16),
            pltpu.VMEM((1, *WEIGHTS["b"]), jnp.bfloat16),
            pltpu.VMEM((2, 2 * T, 384), jnp.float32),
            pltpu.SemaphoreType.DMA((6,)),
            pltpu.SemaphoreType.DMA((2,)),
        ],
        compiler_params=VMEM_LIMIT,
        name="last",
    )(tab, *xs, a, b, ta, tb)


def finish_kernel(
    tab, own_ref, par_ref, inv_ref, cos_ref, sin_ref, mask_ref, x_ref,
    o0, o1, o2, o3, p0, p1, p2, p3, out_ref, ot, ys, mixed, sem, ysem,
):
    core = tab[CORE]
    for at, pieces, c in ((Z, (o0, o1, o2, o3), core), (ZP, (p0, p1, p2, p3), 1 - core)):
        for n, piece in enumerate(pieces):
            for i in range(2):
                z = tab[at + n * 2 + i]
                for y in range(NY):
                    pltpu.make_async_copy(
                        piece.at[i, y], ot.at[y, c, z % NZL, :, z // NZL], sem.at[1]
                    ).start()
    inv, cos, sin = inv_ref[...], cos_ref[...], sin_ref[...]
    allowed = mask_ref[...] > 0

    def raw(col):
        return (own_ref[:, col : col + HD] + par_ref[:, col : col + HD]) * inv

    keys = rope(raw(512), cos, sin).astype(jnp.bfloat16)
    values = raw(640).astype(jnp.bfloat16)
    for h in range(4):
        q = rope(raw(h * HD), cos, sin).astype(jnp.bfloat16)
        s = lax.dot_general(q, keys, (((1,), (1,)), ((), ())), preferred_element_type=jnp.float32)
        s = jnp.where(allowed, s * (1.0 / math.sqrt(HD)), -1e30)
        e = jnp.exp(s - jnp.max(s, -1, keepdims=True))
        probs = (e / jnp.sum(e, -1, keepdims=True)).astype(jnp.bfloat16)
        mixed[:, h * HD : h * HD + HD] = jnp.dot(
            probs, values, preferred_element_type=jnp.float32
        ).astype(jnp.bfloat16)
    pltpu.make_async_copy(ot, ot, sem.at[1]).wait()
    writes = []
    for k in range(NY * NC):
        rows = ot[k // NC, k % NC].reshape(1024, 512)
        branch = lax.dot_general(
            mixed[...], rows, (((1,), (1,)), ((), ())), preferred_element_type=jnp.float32
        )
        ys[k] = (x_ref[k].astype(jnp.float32) + branch).astype(jnp.bfloat16)
        writes.append(pltpu.make_async_copy(ys.at[k], out_ref.at[:, pl.ds(k * 1024, 1024)], ysem.at[k]))
        writes[-1].start()
    for w in writes:
        w.wait()


def body(stream, segment_ids, positions, norm_gain, q_weight, k_weight, v_weight, o_weight):
    gain = norm_gain[0].astype(jnp.float32)[:, None]
    qkv = jnp.concatenate([q_weight[0], k_weight[0], v_weight[0]], -1)
    qkv = lax.optimization_barrier((qkv.astype(jnp.float32) * gain).astype(jnp.bfloat16))

    tab = table()
    smem = pl.BlockSpec(memory_space=pltpu.SMEM)
    vmem = pl.BlockSpec(memory_space=pltpu.VMEM)
    hbm = pl.BlockSpec(memory_space=pl.ANY)

    shape = (NZL, NZH, ROWS, 384)
    a, b = local(arrange_columns_kernel, tab, gather(qkv, "z"), [shape] * 2)
    a, b = spread(a, "x"), spread(b, "y")
    (a,) = local(functools.partial(arrange_kernel, X), tab, a, [(NX, *shape)])
    (b,) = local(functools.partial(arrange_kernel, Y), tab, b, [(NY, *shape)])
    a, b = spread(a, "y"), spread(b, "x")

    o, _ = lax.optimization_barrier((o_weight[0].T, qkv))
    o = jnp.concatenate(gather(o, "x"))
    (o,) = local(arrange_plane_kernel, tab, gather(o, "y"), [(NY, NX, ROWS, 512)])
    o = gather(o, "z")

    def swap(a):
        return lax.ppermute(a, "c", [(0, 1), (1, 0)])

    o_par = [swap(v) for v in o]

    freqs = jnp.exp(-math.log(500000.0) * jnp.arange(HD // 2, dtype=jnp.float32) * 2.0 / HD)
    angles = positions.astype(jnp.float32)[:, None] * freqs[None, :]
    cos, sin = jnp.cos(angles), jnp.sin(angles)
    cos = jnp.concatenate([cos, cos], -1)
    sin = jnp.concatenate([-sin, sin], -1)
    allowed = (segment_ids[:, None] == segment_ids[None, :]) & (positions[None, :] <= positions[:, None])
    mask = allowed.astype(jnp.float32)

    x_par = pl.pallas_call(
        other_half_kernel,
        in_specs=[smem, hbm],
        out_specs=vmem,
        out_shape=jax.ShapeDtypeStruct((T, 4096), jnp.bfloat16),
        scratch_shapes=[pltpu.SemaphoreType.DMA((NY,))],
        compiler_params=VMEM_LIMIT,
        name="other_half",
    )(tab, stream)
    x_par = swap(x_par)
    x_cut = pl.pallas_call(
        prepare_kernel,
        in_specs=[smem, hbm, hbm],
        out_specs=vmem,
        out_shape=jax.ShapeDtypeStruct((4, 2 * T, 1024), jnp.bfloat16),
        scratch_shapes=[
            pltpu.VMEM((4, 2 * T, 1024), jnp.bfloat16),
            pltpu.SemaphoreType.DMA((8,)),
        ],
        compiler_params=VMEM_LIMIT,
        name="prepare",
    )(tab, stream, x_par)
    kept, inv = pl.pallas_call(
        rms_kernel,
        in_specs=[hbm],
        out_specs=[vmem, vmem],
        out_shape=[pltpu.VMEM((8, T, 1024), jnp.bfloat16), jax.ShapeDtypeStruct((T, 1), jnp.float32)],
        scratch_shapes=[pltpu.SemaphoreType.DMA((8,))],
        compiler_params=VMEM_LIMIT,
        name="rms",
    )(stream)
    xs = (stream, x_par, x_cut)
    total_a = first_products("a", tab, xs, a[:3])
    total_b = first_products("b", tab, xs, b[:3])
    own, par = last_products(tab, xs, a[3], b[3], total_a, total_b)
    par = swap(par)
    return pl.pallas_call(
        finish_kernel,
        in_specs=[smem] + [vmem] * 7 + [hbm] * 8,
        out_specs=hbm,
        out_shape=jax.ShapeDtypeStruct((T, 8192), jnp.bfloat16),
        scratch_shapes=[
            pltpu.VMEM((NY, NC, NZL, NX, NZH, ROWS, 512), jnp.bfloat16),
            pltpu.VMEM((NY * NC, T, 1024), jnp.bfloat16),
            pltpu.VMEM((T, 512), jnp.bfloat16),
            pltpu.SemaphoreType.DMA((2,)),
            pltpu.SemaphoreType.DMA((NY * NC,)),
        ],
        compiler_params=VMEM_LIMIT,
        name="finish",
    )(tab, own, par, inv, cos, sin, mask, kept, *o, *o_par)


def solution(mesh):
    fine = Mesh(mesh.devices.reshape(NY, NC, NZL, NX, NZH), AXES)
    in_specs = (
        P(AXES, None),
        P(AXES),
        P(AXES),
        P(None, AXES),
        P(None, AXES, None),
        P(None, AXES, None),
        P(None, AXES, None),
        P(None, None, AXES),
    )

    return jax.shard_map(body, mesh=fine, in_specs=in_specs, out_specs=P(AXES, None), check_vma=False)
```
